32 devices in a mesh: row: 16 (over z, x, core), ch: 2 (over y).
Axes of the slice: x: 2, y: 2, z: 4, core: 2. Of those that a mesh axis runs over, the one named last changes fastest.
Arguments:
- pair_rep: float32 [256, 256, 128], P('row', 'ch'), may hold values from -6 to 6
- residue_mask: int32 [256], replicated, may hold values 0 or 1
- pair_gain: float32 [2, 128], replicated, may hold values from 0.5 to 1.5
- pair_shift: float32 [2, 128], replicated, may hold values from -3 to 3
- panel_weight: bfloat16 [2, 128, 512], replicated, may hold values from -0.5 to 0.5
- panel_bias: float32 [2, 512], replicated, may hold values from -3 to 3
- gate_weight: bfloat16 [2, 128, 128], replicated, may hold values from -0.5 to 0.5
- gate_bias: float32 [2, 128], replicated, may hold values from -3 to 3
- hidden_gain: float32 [2, 128], replicated, may hold values from 0.5 to 1.5
- hidden_shift: float32 [2, 128], replicated, may hold values from -3 to 3
- output_weight: bfloat16 [2, 128, 128], replicated, may hold values from -0.5 to 0.5
- output_bias: float32 [2, 128], replicated, may hold values from -3 to 3
Outputs:
- updated_pair: float32 [256, 256, 128], P('row', 'ch')
The draws below stay inside these ranges and needn't reach their ends.
All inputs are finite; a program needn't handle non-finite values.
Results may differ from the reference program's by a relative error of at most 0.0039.
Values may be sent and summed in bfloat16 or wider, within the bound.
A program may use at most 64 MiB of HBM per device.

```python
import math
import jax
import jax.numpy as jnp
from jax import lax

C = 128
H = 128
N = 256


def place_ends(array, rng, low, largest):
    spot = [jax.random.randint(jax.random.fold_in(rng, axis), (), 0, length) for axis, length in enumerate(array.shape)]
    widest = array.shape.index(max(array.shape))
    neighbour = spot[:widest] + [(spot[widest] + 1) % array.shape[widest]] + spot[widest + 1:]
    return array.at[tuple(spot)].set(low).at[tuple(neighbour)].set(largest)


def levels(own_key, extent, cuts, smallest, top_value):
    factor_of, own = 1.0, jax.random.fold_in(own_key, 6)
    for axis_at, parts in cuts:
        steps = jnp.exp(jax.random.uniform(jax.random.fold_in(own, axis_at), (parts,), jnp.float32, smallest / len(cuts), top_value / len(cuts)))
        factor_of = factor_of * jnp.repeat(steps, extent[axis_at] // parts).reshape([-1 if axis == axis_at else 1 for axis in range(len(extent))])
    return factor_of


def noise(stream_key, dims, scale, most, cuts=(), kind=jnp.bfloat16):
    array = jax.random.normal(stream_key, dims, jnp.float32) * scale
    if len(cuts) > 0:
        array = levels(stream_key, dims, cuts, -0.22, 0.18) * array
    return jnp.clip(array, min=-most, max=most).astype(kind)


def setup_inputs(seed: int = 0) -> dict:
    key_of = jax.random.split(jax.random.key(seed), 13)
    pair_rep = noise(key_of[0], (N, N, C), 1.0, 6.0, ((0, 16), (1, 2)), jnp.float32)
    residue_mask = place_ends((jax.random.randint(key_of[1], (N,), 0, 8) < 7).astype(jnp.int32), jax.random.fold_in(key_of[1], 1), 0, 1)
    pair_gain = jnp.clip(jax.random.uniform(key_of[2], (2, C), jnp.float32, 0.5, 1.5), 0.5, 1.5)
    pair_shift = noise(key_of[3], (2, C), 0.5, 3.0, (), jnp.float32)
    panel_weight = noise(key_of[4], (2, C, 4 * H), C ** -0.5, 0.5)
    panel_bias = noise(key_of[5], (2, 4 * H), 0.5, 3.0, (), jnp.float32)
    gate_weight = noise(key_of[6], (2, C, C), C ** -0.5, 0.5)
    gate_bias = noise(key_of[7], (2, C), 0.5, 3.0, (), jnp.float32)
    hidden_gain = jnp.clip(jax.random.uniform(key_of[8], (2, H), jnp.float32, 0.5, 1.5), 0.5, 1.5)
    hidden_shift = noise(key_of[9], (2, H), 0.5, 3.0, (), jnp.float32)
    output_weight = noise(key_of[10], (2, H, C), H ** -0.5, 0.5)
    output_bias = noise(key_of[11], (2, C), 0.5, 3.0, (), jnp.float32)
    return dict(pair_rep=pair_rep, residue_mask=residue_mask, pair_gain=pair_gain, pair_shift=pair_shift, panel_weight=panel_weight, panel_bias=panel_bias, gate_weight=gate_weight, gate_bias=gate_bias, hidden_gain=hidden_gain, hidden_shift=hidden_shift, output_weight=output_weight, output_bias=output_bias)


PAIR_EPSILON = 1e-05
HIDDEN_EPSILON = 1.0

def layer_norm(values, gain_value, shift_value, along, epsilon):
    center = lax.optimization_barrier(jnp.mean(values, axis=along, keepdims=True))
    offset = values - center
    spread = lax.optimization_barrier(jnp.mean(offset * offset, axis=along, keepdims=True))
    return offset * lax.rsqrt(spread + epsilon) * gain_value + shift_value

def update(current, cell_mask, section_index, pair_gain, pair_shift, panel_weight, panel_bias, gate_weight, gate_bias, hidden_gain, hidden_shift, output_weight, output_bias):
    normed = layer_norm(current, pair_gain[section_index], pair_shift[section_index], -1, PAIR_EPSILON).astype(jnp.bfloat16)
    flattened = normed.reshape(N * N, C)
    weight = panel_weight[section_index]
    biases = panel_bias[section_index]

    def column(which_one):
        result = jnp.dot(flattened, weight[:, which_one * H:(which_one + 1) * H], preferred_element_type=jnp.float32)
        return (result + biases[which_one * H:(which_one + 1) * H]).reshape(N, N, H)
    left_panel = (cell_mask[:, :, None] * jax.nn.sigmoid(column(0)) * column(1)).astype(jnp.bfloat16)
    right_panel = (cell_mask[:, :, None] * jax.nn.sigmoid(column(2)) * column(3)).astype(jnp.bfloat16)
    gate_value = jax.nn.sigmoid(jnp.dot(flattened, gate_weight[section_index], preferred_element_type=jnp.float32) + gate_bias[section_index]).reshape(N, N, C)
    if section_index == 1:
        left_panel = jnp.transpose(left_panel, (1, 0, 2))
        right_panel = jnp.transpose(right_panel, (1, 0, 2))
    left_hidden = jnp.transpose(left_panel, (2, 0, 1)).astype(jnp.float32)
    right_hidden = jnp.transpose(right_panel, (2, 0, 1)).astype(jnp.float32)
    block_rows = math.gcd(N, 128)
    block_count = N // block_rows
    out_weight = output_weight[section_index].astype(jnp.float32)

    def one_block(block_index):
        row_start = block_index * block_rows
        left_rows = lax.dynamic_slice_in_dim(left_hidden, row_start, block_rows, 1)
        products = jnp.einsum('hik,hjk->hij', left_rows, right_hidden, precision=lax.Precision.HIGHEST)
        normed_hidden = layer_norm(products, hidden_gain[section_index][:, None, None], hidden_shift[section_index][:, None, None], 0, HIDDEN_EPSILON).astype(jnp.bfloat16)
        projected = jnp.einsum('hij,hc->ijc', normed_hidden.astype(jnp.float32), out_weight, precision=lax.Precision.HIGHEST)
        gate_rows = lax.dynamic_slice_in_dim(gate_value, row_start, block_rows, 0)
        return gate_rows * (projected + output_bias[section_index])
    updates = lax.map(one_block, jnp.arange(block_count, dtype=jnp.int32))
    return current + updates.reshape(N, N, C)

def reference(pair_rep, residue_mask, pair_gain, pair_shift, panel_weight, panel_bias, gate_weight, gate_bias, hidden_gain, hidden_shift, output_weight, output_bias):
    residue_float = residue_mask.astype(jnp.float32)
    cell_mask = residue_float[:, None] * residue_float[None, :]
    current = pair_rep
    for section_index in range(2):
        current = update(current, cell_mask, section_index, pair_gain, pair_shift, panel_weight, panel_bias, gate_weight, gate_bias, hidden_gain, hidden_shift, output_weight, output_bias)
    return current
```

```python
import functools

import jax
import jax.numpy as jnp
from jax import lax
from jax.experimental import pallas as pl
from jax.experimental.pallas import tpu as pltpu
from jax.sharding import PartitionSpec as P

PAIR_EPSILON = 1e-05
HIDDEN_EPSILON = 1.0
MESH = pl.DeviceIdType.MESH


def kernel(
    sizes,
    pair_ref,
    mask_smem,
    mask_ref,
    pair_gain,
    pair_shift,
    panel_weight,
    panel_bias,
    gate_weight,
    gate_bias,
    hidden_gain,
    hidden_shift,
    output_weight,
    output_bias,
    out_ref,
    weight_t,
    bias_t,
    stage,
    send_ab,
    recv_a,
    recv_b,
    send_x,
    recv_x,
    gate,
    ab_send_sem,
    ab_recv_sem,
    x_send_sem,
    x_recv_sem,
):
    rows, cols, hidden, row_total, col_total, per_slot, quarters = sizes
    devices = row_total * col_total
    group = hidden // col_total
    total = row_total * rows
    part = total // quarters
    my_row = lax.axis_index("row")
    my_col = lax.axis_index("ch")
    me = my_row * col_total + my_col

    def peer_of(step):
        half = (step + 1) // 2
        turn = devices // 2 + half * (1 - 2 * (step % 2)) + devices
        peer = lax.rem(me + turn, devices)
        return peer // col_total, lax.rem(peer, col_total)

    barrier = pltpu.get_barrier_semaphore()

    def greet(step, carry):
        peer_row, peer_col = peer_of(step)
        pl.semaphore_signal(barrier, inc=1, device_id=(peer_row, peer_col), device_id_type=MESH)
        return carry

    lax.fori_loop(0, devices - 1, greet, 0)

    def hidden_offset(row, col):
        return col * group + (row // quarters) * per_slot

    def ab_refs(section, which, row, col):
        source = send_ab.at[section, which, pl.ds(hidden_offset(row, col), per_slot)]
        row_at = pl.multiple_of(my_row * rows, rows)
        col_at = pl.multiple_of(my_col * cols, cols)
        if which == 0:
            if section == 0:
                row_at = pl.multiple_of(lax.rem(row_at, part), rows)
                target = recv_a[0].at[:, pl.ds(row_at, rows), pl.ds(col_at, cols)]
            else:
                col_at = pl.multiple_of(lax.rem(col_at, part), cols)
                target = recv_a[1].at[:, pl.ds(row_at, rows), pl.ds(col_at, cols)]
        else:
            target = recv_b.at[section, :, pl.ds(row_at, rows), pl.ds(col_at, cols)]
        return source, target

    def my_part(section):
        return my_row * rows // part if section == 0 else my_col * cols // part

    def ab_copies(section, step, act):
        peer_row, peer_col = peer_of(step)
        for which in range(2):
            source, target = ab_refs(section, which, peer_row, peer_col)
            copy = pltpu.make_async_remote_copy(
                src_ref=source,
                dst_ref=target,
                send_sem=ab_send_sem.at[section, which],
                recv_sem=ab_recv_sem.at[section, which],
                device_id=(peer_row, peer_col),
                device_id_type=MESH,
            )
            if which == 0 and quarters > 1:
                pl.when(lax.rem(peer_row, quarters) == my_part(section))(functools.partial(act, copy))
            else:
                act(copy)

    def ab_own(section):
        for which in range(2):
            source, target = ab_refs(section, which, my_row, my_col)
            copy = pltpu.make_async_copy(source, target, ab_recv_sem.at[section, which])
            if which == 0 and quarters > 1:
                pl.when(lax.rem(my_row, quarters) == my_part(section))(copy.start)
            else:
                copy.start()

    def x_refs(section, row, col):
        row_at = pl.multiple_of(lax.rem(row * rows, part), rows)
        col_at = pl.multiple_of(col * cols, cols)
        source = send_x.at[section, :, pl.ds(row_at, rows), pl.ds(col_at, cols)]
        target = recv_x.at[section, pl.ds(hidden_offset(my_row, my_col), per_slot)]
        return source, target

    def x_copies(section, step, act):
        peer_row, peer_col = peer_of(step)
        source, target = x_refs(section, peer_row, peer_col)
        copy = pltpu.make_async_remote_copy(
            src_ref=source,
            dst_ref=target,
            send_sem=x_send_sem.at[section],
            recv_sem=x_recv_sem.at[section],
            device_id=(peer_row, peer_col),
            device_id_type=MESH,
        )
        if quarters > 1:
            pl.when(peer_row * rows // part == lax.rem(my_row, quarters))(functools.partial(act, copy))
        else:
            act(copy)

    def x_own(section):
        source, target = x_refs(section, my_row, my_col)
        copy = pltpu.make_async_copy(source, target, x_recv_sem.at[section])
        if quarters > 1:
            pl.when(my_row * rows // part == lax.rem(my_row, quarters))(copy.start)
        else:
            copy.start()

    def every_peer(body):
        def step_body(step, carry):
            body(step)
            return carry

        lax.fori_loop(0, devices - 1, step_body, 0)

    start = lambda copy: copy.start()
    wait_send = lambda copy: copy.wait_send()

    def wait_all(ref, sem):
        pltpu.make_async_copy(ref, ref, sem).wait()

    col_mask = mask_ref[pl.ds(my_col, 1), :].astype(jnp.float32)

    for section in range(2):
        current = pair_ref if section == 0 else out_ref
        weight_t[...] = panel_weight[section].astype(jnp.float32).T.astype(jnp.bfloat16)
        bias_t[...] = jnp.broadcast_to(panel_bias[pl.ds(section, 1), :], (cols, 4 * hidden)).T
        gain_row = pair_gain[pl.ds(section, 1), :]
        shift_row = pair_shift[pl.ds(section, 1), :]

        def project(r, carry):
            values = current[r]
            offset = values - jnp.mean(values, axis=1, keepdims=True)
            spread = jnp.mean(offset * offset, axis=1, keepdims=True)
            normed = offset * lax.rsqrt(spread + PAIR_EPSILON) * gain_row + shift_row
            normed = normed.astype(jnp.bfloat16)
            mask = col_mask * mask_smem[my_row * rows + r].astype(jnp.float32)
            for which in range(2):
                base = 2 * which * hidden
                features = lax.dot_general(
                    weight_t[pl.ds(base, 2 * hidden), :],
                    normed,
                    (((1,), (1,)), ((), ())),
                    preferred_element_type=jnp.float32,
                )
                features = features + bias_t[pl.ds(base, 2 * hidden), :]
                panel = mask * jax.nn.sigmoid(features[:hidden]) * features[hidden:]
                stage[which, pl.ds(r, hidden, stride=rows), :] = panel
            gate[r] = jax.nn.sigmoid(
                jnp.dot(normed, gate_weight[section], preferred_element_type=jnp.float32)
                + gate_bias[pl.ds(section, 1), :]
            )
            return carry

        lax.fori_loop(0, rows, project, 0)
        for which in range(2):
            send_ab[section, which] = (
                stage[which].astype(jnp.bfloat16).reshape(hidden, rows, cols)
            )
        if section == 0:
            pl.semaphore_wait(barrier, devices - 1)
        every_peer(lambda step: ab_copies(section, step, start))
        ab_own(section)
        wait_all(recv_a[section], ab_recv_sem.at[section, 0])
        wait_all(recv_b.at[section], ab_recv_sem.at[section, 1])
        for h in range(per_slot):
            left, right = recv_a[section][h], recv_b[section, h]
            contract = 1 if section == 0 else 0
            send_x[section, h] = lax.dot_general(
                left,
                right,
                (((contract,), (contract,)), ((), ())),
                preferred_element_type=jnp.float32,
            ).astype(jnp.bfloat16)
        every_peer(lambda step: x_copies(section, step, start))
        x_own(section)
        gain_t = jnp.broadcast_to(hidden_gain[pl.ds(section, 1), :], (cols, hidden)).T
        shift_t = jnp.broadcast_to(hidden_shift[pl.ds(section, 1), :], (cols, hidden)).T
        bias_t[pl.ds(0, hidden), :] = gain_t
        bias_t[pl.ds(hidden, hidden), :] = shift_t
        wait_all(recv_x.at[section], x_recv_sem.at[section])
        stage[0] = recv_x[section].reshape(hidden * rows, cols).astype(jnp.float32)

        def finish(r, carry):
            values = stage[0, pl.ds(r, hidden, stride=rows), :]
            offset = values - jnp.mean(values, axis=0, keepdims=True)
            spread = jnp.mean(offset * offset, axis=0, keepdims=True)
            normed = offset * lax.rsqrt(spread + HIDDEN_EPSILON) * bias_t[pl.ds(0, hidden), :]
            normed = (normed + bias_t[pl.ds(hidden, hidden), :]).astype(jnp.bfloat16)
            projected = lax.dot_general(
                normed,
                output_weight[section],
                (((0,), (0,)), ((), ())),
                preferred_element_type=jnp.float32,
            )
            out_ref[r] = current[r] + gate[r] * (projected + output_bias[pl.ds(section, 1), :])
            return carry

        lax.fori_loop(0, rows, finish, 0)

    for section in range(2):
        if quarters == 1:
            sent = hidden - per_slot
            for which in range(2):
                wait_all(send_ab.at[section, which, pl.ds(0, sent)], ab_send_sem.at[section, which])
            wait_all(recv_x.at[section, pl.ds(0, sent)], x_send_sem.at[section])
        else:
            every_peer(lambda step: ab_copies(section, step, wait_send))
            every_peer(lambda step: x_copies(section, step, wait_send))


def local(row_total, col_total, pair_rep, residue_mask, *parameters):
    rows, cols, channels = pair_rep.shape
    hidden = parameters[2].shape[2] // 4
    group = hidden // col_total
    per_slot, quarters = (group // row_total, 1) if group >= row_total else (1, row_total // group)
    total = row_total * rows
    part = total // quarters
    sizes = (rows, cols, hidden, row_total, col_total, per_slot, quarters)
    vmem = pl.BlockSpec(memory_space=pltpu.VMEM)
    smem = pl.BlockSpec(memory_space=pltpu.SMEM)
    bf16, f32 = jnp.bfloat16, jnp.float32

    def body(*refs):
        refs = list(refs)
        at = 14 + 5
        recv_a = (refs[at - 1], refs[at])
        merged = refs[: at - 1] + [recv_a] + refs[at + 1 :]
        kernel(sizes, *merged)

    return pl.pallas_call(
        body,
        out_shape=jax.ShapeDtypeStruct((rows, cols, channels), f32),
        in_specs=[vmem, smem] + [vmem] * 11,
        out_specs=vmem,
        scratch_shapes=[
            pltpu.VMEM((4 * hidden, channels), bf16),
            pltpu.VMEM((4 * hidden, cols), f32),
            pltpu.VMEM((2, hidden * rows, cols), f32),
            pltpu.VMEM((2, 2, hidden, rows, cols), bf16),
            pltpu.VMEM((per_slot, part, total), bf16),
            pltpu.VMEM((per_slot, total, part), bf16),
            pltpu.VMEM((2, per_slot, total, total), bf16),
            pltpu.VMEM((2, per_slot, part, total), bf16),
            pltpu.VMEM((2, hidden, rows, cols), bf16),
            pltpu.VMEM((rows, cols, channels), f32),
            pltpu.SemaphoreType.DMA((2, 2)),
            pltpu.SemaphoreType.DMA((2, 2)),
            pltpu.SemaphoreType.DMA((2,)),
            pltpu.SemaphoreType.DMA((2,)),
        ],
        compiler_params=pltpu.CompilerParams(
            collective_id=0, has_side_effects=True, vmem_limit_bytes=48 * 1024 * 1024
        ),
    )(pair_rep, residue_mask, residue_mask.reshape(col_total, cols), *parameters)


def solution(mesh):
    return jax.shard_map(
        functools.partial(local, mesh.shape["row"], mesh.shape["ch"]),
        mesh=mesh,
        in_specs=(P("row", "ch", None), P(), P(), P(), P(), P(), P(), P(), P(), P(), P(), P()),
        out_specs=P("row", "ch", None),
        check_vma=False,
    )
```

```python
import functools

import jax
import jax.numpy as jnp
from jax import lax
from jax.experimental import pallas as pl
from jax.experimental.pallas import tpu as pltpu
from jax.sharding import PartitionSpec as P

PAIR_EPSILON = 1e-05
HIDDEN_EPSILON = 1.0
MESH = pl.DeviceIdType.MESH
CHUNKS = 4
NAMES = (
    "pair",
    "mask",
    "pair_gain",
    "pair_shift",
    "panel_weight",
    "panel_bias",
    "gate_weight",
    "gate_bias",
    "hidden_gain",
    "hidden_shift",
    "output_weight",
    "output_bias",
)


def normalize(values, axis, epsilon, gain, shift):
    offset = values - jnp.mean(values, axis=axis, keepdims=True)
    spread = jnp.mean(offset * offset, axis=axis, keepdims=True)
    return (offset * lax.rsqrt(spread + epsilon) * gain + shift).astype(jnp.bfloat16)


def kernel(sizes, mask_smem, *refs):
    rows, cols, hidden, row_total, col_total, parts, chunks = sizes
    count = len(NAMES)
    sources = dict(zip(NAMES, refs[:count]))
    out_ref = refs[count]
    held = dict(zip(NAMES, refs[count + 1 : 2 * count + 1]))
    (
        weight_t,
        bias_t,
        affine_t,
        normed_ref,
        stage,
        stage_x,
        gate,
        send_ab,
        recv_a,
        recv_b,
        recv_ab,
        send_x0,
        send_x1,
        recv_x0,
        recv_x1,
        load_sem,
        a_send_sem,
        a_recv_sem,
        b_send_sem,
        b_recv_sem,
        ab_send_sem,
        ab_recv_sem,
        x_send_sem,
        x_recv_sem,
    ) = refs[2 * count + 1 :]
    devices = row_total * col_total
    row_part = row_total // parts
    members = row_part * col_total
    per_slot = hidden // members
    piece = per_slot // chunks
    wide = hidden // chunks
    total = row_total * rows
    part = total // parts
    my_row = lax.axis_index("row")
    my_col = lax.axis_index("ch")
    my_group = my_row // row_part
    my_place = lax.rem(my_row, row_part) * col_total + my_col

    loads = [
        pltpu.make_async_copy(sources[name], held[name], load_sem.at[at])
        for at, name in enumerate(NAMES)
    ]
    for load in loads:
        load.start()

    def partner(distance, step):
        group = lax.rem(my_group + distance, parts)
        place = lax.rem(my_place + step, members)
        return group * row_part + place // col_total, lax.rem(place, col_total), place

    def each(first, body):
        def step_body(step, carry):
            body(step)
            return carry

        lax.fori_loop(first, members, step_body, 0)

    barrier = pltpu.get_barrier_semaphore()
    for distance in range(parts):

        def greet(step):
            row, col, _ = partner(distance, step)
            pl.semaphore_signal(barrier, inc=1, device_id=(row, col), device_id_type=MESH)

        each(1 if distance == 0 else 0, greet)

    def wait_bytes(ref, sem):
        pltpu.make_async_copy(ref, ref, sem).wait()

    def remote(source, target, send_sem, recv_sem, row, col):
        pltpu.make_async_remote_copy(
            src_ref=source,
            dst_ref=target,
            send_sem=send_sem,
            recv_sem=recv_sem,
            device_id=(row, col),
            device_id_type=MESH,
        ).start()

    row_at = pl.multiple_of(my_row * rows, rows)
    near_at = pl.multiple_of(lax.rem(my_row, row_part) * rows, rows)
    col_at = pl.multiple_of(my_col * cols, cols)

    def panels(chunk, place):
        return pl.ds(chunk * wide + place * piece, piece)

    def send_panels(section, chunk):
        spot = pl.ds(chunk * piece, piece)
        if section == 0:
            a_to = recv_a.at[spot, pl.ds(near_at, rows), pl.ds(col_at, cols)]
            b_to = recv_b.at[spot, pl.ds(row_at, rows), pl.ds(col_at, cols)]

            def far(distance, step):
                row, col, place = partner(distance, step)
                source = send_ab.at[0, 1, panels(chunk, place)]
                remote(
                    source, b_to, b_send_sem.at[distance], b_recv_sem.at[chunk], row, col
                )

            def near(step):
                row, col, place = partner(0, step)
                source = send_ab.at[0, 0, panels(chunk, place)]
                remote(source, a_to, a_send_sem, a_recv_sem.at[chunk], row, col)

            for distance in range(parts - 1, -1, -1):
                each(1 if distance == 0 else 0, functools.partial(far, distance))
            each(1, near)
            own = panels(chunk, my_place)
            pltpu.make_async_copy(send_ab.at[0, 0, own], a_to, a_recv_sem.at[chunk]).start()
            pltpu.make_async_copy(send_ab.at[0, 1, own], b_to, b_recv_sem.at[chunk]).start()
        else:
            to = recv_ab.at[:, spot, pl.ds(near_at, rows), pl.ds(col_at, cols)]

            def both(step):
                row, col, place = partner(0, step)
                source = send_ab.at[1, :, panels(chunk, place)]
                remote(source, to, ab_send_sem, ab_recv_sem.at[chunk], row, col)

            each(1, both)
            own = send_ab.at[1, :, panels(chunk, my_place)]
            pltpu.make_async_copy(own, to, ab_recv_sem.at[chunk]).start()

    def wait_panels(section, chunk):
        spot = pl.ds(chunk * piece, piece)
        if section == 0:
            wait_bytes(recv_a.at[spot], a_recv_sem.at[chunk])
            wait_bytes(recv_b.at[spot], b_recv_sem.at[chunk])
        else:
            wait_bytes(recv_ab.at[:, spot], ab_recv_sem.at[chunk])

    def send_products(section, chunk):
        spot = pl.ds(chunk * piece, piece)
        lands = panels(chunk, my_place)

        def refs_of(row, col):
            to_row = row if section == 1 else lax.rem(row, row_part)
            at = pl.ds(pl.multiple_of(to_row * rows, rows), rows)
            along = pl.ds(pl.multiple_of(col * cols, cols), cols)
            if section == 0:
                return send_x0.at[spot, at, along], recv_x0.at[lands]
            return send_x1.at[spot, at, along], recv_x1.at[my_group, lands]

        def other(distance, step):
            row, col, _ = partner(distance, step)
            source, target = refs_of(row, col)
            remote(
                source,
                target,
                x_send_sem.at[section, distance],
                x_recv_sem.at[section, chunk],
                row,
                col,
            )

        for distance in range(parts - 1 if section == 1 else 0, -1, -1):
            each(1 if distance == 0 else 0, functools.partial(other, distance))
        source, target = refs_of(my_row, my_col)
        pltpu.make_async_copy(source, target, x_recv_sem.at[section, chunk]).start()

    def prepare(section):
        for block in range(4):
            span = slice(block * hidden, (block + 1) * hidden)
            turned = held["panel_weight"][section, :, span].astype(jnp.float32).T
            turned = turned.astype(jnp.bfloat16)
            biases = held["panel_bias"][pl.ds(section, 1), span]
            biases = jnp.broadcast_to(biases, (cols, hidden)).T
            for chunk in range(chunks):
                to = pl.ds((chunk * 4 + block) * wide, wide)
                weight_t[section, to, :] = turned[chunk * wide : (chunk + 1) * wide]
                bias_t[section, to, :] = biases[chunk * wide : (chunk + 1) * wide]
        for at, name in enumerate(("hidden_gain", "hidden_shift")):
            line = held[name][pl.ds(section, 1), :]
            affine_t[section, at] = jnp.broadcast_to(line, (cols, hidden)).T

    def norm_row(section, values):
        return normalize(
            values,
            1,
            PAIR_EPSILON,
            held["pair_gain"][pl.ds(section, 1), :],
            held["pair_shift"][pl.ds(section, 1), :],
        )

    for load in loads:
        load.wait()
    prepare(0)

    def first_norm(r, carry):
        normed_ref[r] = norm_row(0, held["pair"][r])
        return carry

    lax.fori_loop(0, rows, first_norm, 0, unroll=4)
    col_mask = held["mask"][pl.ds(my_col, 1), :].astype(jnp.float32)

    for section in range(2):
        current = held["pair"] if section == 0 else out_ref
        for chunk in range(chunks):

            def project(r, carry):
                span = pl.ds(chunk * 4 * wide, 4 * wide)
                features = lax.dot_general(
                    weight_t[section, span, :],
                    normed_ref[r],
                    (((1,), (1,)), ((), ())),
                    preferred_element_type=jnp.float32,
                )
                features = features + bias_t[section, span, :]
                mask = col_mask * mask_smem[my_row * rows + r].astype(jnp.float32)
                for which in range(2):
                    at = 2 * which * wide
                    panel = mask * jax.nn.sigmoid(features[at : at + wide])
                    panel = panel * features[at + wide : at + 2 * wide]
                    stage[which, pl.ds(r, wide, stride=rows), :] = panel
                return carry

            lax.fori_loop(0, rows, project, 0, unroll=4)
            for which in range(2):
                send_ab[section, which, pl.ds(chunk * wide, wide)] = (
                    stage[which].astype(jnp.bfloat16).reshape(wide, rows, cols)
                )
            if section == 0 and chunk == 0:
                pl.semaphore_wait(barrier, devices - 1)
            send_panels(section, chunk)

        def gates(r, carry):
            gate[r] = jax.nn.sigmoid(
                jnp.dot(
                    normed_ref[r],
                    held["gate_weight"][section],
                    preferred_element_type=jnp.float32,
                )
                + held["gate_bias"][pl.ds(section, 1), :]
            )
            return carry

        lax.fori_loop(0, rows, gates, 0, unroll=4)
        if section == 0:
            prepare(1)
        for chunk in range(chunks):
            wait_panels(section, chunk)
            for h in range(chunk * piece, (chunk + 1) * piece):
                if section == 0:
                    left, right, along, to = recv_a[h], recv_b[h], 1, send_x0
                else:
                    left, right, along, to = recv_ab[0, h], recv_ab[1, h], 0, send_x1
                to[h] = lax.dot_general(
                    left,
                    right,
                    (((along,), (along,)), ((), ())),
                    preferred_element_type=jnp.float32,
                ).astype(jnp.bfloat16)
            send_products(section, chunk)
        for chunk in range(chunks):
            spot = pl.ds(chunk * wide, wide)
            if section == 0:
                wait_bytes(recv_x0.at[spot], x_recv_sem.at[0, chunk])
                got = recv_x0[spot].astype(jnp.float32)
            else:
                wait_bytes(recv_x1.at[:, spot], x_recv_sem.at[1, chunk])
                got = recv_x1[0, spot].astype(jnp.float32)
                for other in range(1, parts):
                    got = got + recv_x1[other, spot].astype(jnp.float32)
            stage_x[pl.ds(chunk * wide * rows, wide * rows), :] = got.reshape(wide * rows, cols)

        def finish(r, carry):
            normed = normalize(
                stage_x[pl.ds(r, hidden, stride=rows), :],
                0,
                HIDDEN_EPSILON,
                affine_t[section, 0],
                affine_t[section, 1],
            )
            projected = lax.dot_general(
                normed,
                held["output_weight"][section],
                (((0,), (0,)), ((), ())),
                preferred_element_type=jnp.float32,
            )
            projected = projected + held["output_bias"][pl.ds(section, 1), :]
            updated = current[r] + gate[r] * projected
            out_ref[r] = updated
            if section == 0:
                normed_ref[r] = norm_row(1, updated)
            return carry

        lax.fori_loop(0, rows, finish, 0, unroll=4)

    one = hidden - per_slot
    wait_bytes(send_ab.at[0, 0, pl.ds(0, one)], a_send_sem)
    wait_bytes(send_ab.at[1, :, pl.ds(0, one)], ab_send_sem)
    for distance in range(parts):
        amount = one if distance == 0 else hidden
        wait_bytes(send_ab.at[0, 1, pl.ds(0, amount)], b_send_sem.at[distance])
        wait_bytes(send_ab.at[0, 1, pl.ds(0, amount)], x_send_sem.at[1, distance])
    wait_bytes(recv_x0.at[pl.ds(0, one)], x_send_sem.at[0, 0])


def local(row_total, col_total, pair_rep, residue_mask, *parameters):
    rows, cols, channels = pair_rep.shape
    hidden = parameters[2].shape[2] // 4
    parts = max(2, row_total * col_total // hidden)
    members = row_total * col_total // parts
    per_slot = hidden // members
    chunks = min(CHUNKS, per_slot)
    wide = hidden // chunks
    total = row_total * rows
    part = total // parts
    sizes = (rows, cols, hidden, row_total, col_total, parts, chunks)
    bf16, f32 = jnp.bfloat16, jnp.float32
    dma = pltpu.SemaphoreType.DMA
    arrays = (pair_rep, residue_mask.reshape(col_total, cols), *parameters)
    return pl.pallas_call(
        functools.partial(kernel, sizes),
        out_shape=jax.ShapeDtypeStruct((rows, cols, channels), f32),
        in_specs=[pl.BlockSpec(memory_space=pltpu.SMEM)]
        + [pl.BlockSpec(memory_space=pltpu.HBM)] * len(arrays),
        out_specs=pl.BlockSpec(memory_space=pltpu.VMEM),
        scratch_shapes=[pltpu.VMEM(array.shape, array.dtype) for array in arrays]
        + [
            pltpu.VMEM((2, 4 * hidden, channels), bf16),
            pltpu.VMEM((2, 4 * hidden, cols), f32),
            pltpu.VMEM((2, 2, hidden, cols), f32),
            pltpu.VMEM((rows, cols, channels), bf16),
            pltpu.VMEM((2, wide * rows, cols), f32),
            pltpu.VMEM((hidden * rows, cols), f32),
            pltpu.VMEM((rows, cols, channels), f32),
            pltpu.VMEM((2, 2, hidden, rows, cols), bf16),
            pltpu.VMEM((per_slot, part, total), bf16),
            pltpu.VMEM((per_slot, total, total), bf16),
            pltpu.VMEM((2, per_slot, part, total), bf16),
            pltpu.VMEM((per_slot, part, total), bf16),
            pltpu.VMEM((per_slot, total, total), bf16),
            pltpu.VMEM((hidden, rows, cols), bf16),
            pltpu.VMEM((parts, hidden, rows, cols), bf16),
            dma((len(arrays),)),
            dma(()),
            dma((chunks,)),
            dma((parts,)),
            dma((chunks,)),
            dma(()),
            dma((chunks,)),
            dma((2, parts)),
            dma((2, chunks)),
        ],
        compiler_params=pltpu.CompilerParams(collective_id=0, has_side_effects=True),
    )(residue_mask, *arrays)


def solution(mesh):
    return jax.shard_map(
        functools.partial(local, mesh.shape["row"], mesh.shape["ch"]),
        mesh=mesh,
        in_specs=(P("row", "ch", None), P(), P(), P(), P(), P(), P(), P(), P(), P(), P(), P()),
        out_specs=P("row", "ch", None),
        check_vma=False,
    )
```

```python
import functools

import jax
import jax.numpy as jnp
from jax import lax
from jax.experimental import pallas as pl
from jax.experimental.pallas import tpu as pltpu
from jax.sharding import PartitionSpec as P

PAIR_EPSILON = 1e-05
HIDDEN_EPSILON = 1.0
MESH = pl.DeviceIdType.MESH
CHUNKS = 4
LEAD = 3
NAMES = (
    "pair",
    "mask",
    "pair_gain",
    "pair_shift",
    "panel_weight",
    "panel_bias",
    "gate_weight",
    "gate_bias",
    "hidden_gain",
    "hidden_shift",
    "output_weight",
    "output_bias",
)


def normalize(values, axis, epsilon, gain, shift):
    offset = values - jnp.mean(values, axis=axis, keepdims=True)
    spread = jnp.mean(offset * offset, axis=axis, keepdims=True)
    return (offset * lax.rsqrt(spread + epsilon) * gain + shift).astype(jnp.bfloat16)


def kernel(sizes, mask_smem, *refs):
    rows, cols, hidden, row_total, col_total, parts, chunks = sizes
    count = len(NAMES)
    sources = dict(zip(NAMES, refs[:count]))
    out_ref = refs[count]
    held = dict(zip(NAMES, refs[count + 1 : 2 * count + 1]))
    (
        weight_t,
        bias_t,
        affine_t,
        normed_ref,
        stage,
        stage_x,
        gate,
        send_ab,
        recv_a,
        recv_b,
        recv_ab,
        send_x0,
        send_x1,
        recv_x0,
        recv_x1,
        load_sem,
        a_send_sem,
        a_recv_sem,
        b_send_sem,
        b_recv_sem,
        ab_send_sem,
        ab_recv_sem,
        x_send_sem,
        x_recv_sem,
    ) = refs[2 * count + 1 :]
    devices = row_total * col_total
    row_part = row_total // parts
    members = row_part * col_total
    per_slot = hidden // members
    piece = per_slot // chunks
    wide = hidden // chunks
    total = row_total * rows
    part = total // parts
    my_row = lax.axis_index("row")
    my_col = lax.axis_index("ch")
    my_group = my_row // row_part
    my_place = lax.rem(my_row, row_part) * col_total + my_col

    loads = [
        pltpu.make_async_copy(sources[name], held[name], load_sem.at[at])
        for at, name in enumerate(NAMES)
    ]
    for load in loads:
        load.start()

    def partner(distance, step):
        group = lax.rem(my_group + distance, parts)
        place = lax.rem(my_place + step, members)
        return group * row_part + place // col_total, lax.rem(place, col_total), place

    def each(first, body):
        def step_body(step, carry):
            body(step)
            return carry

        lax.fori_loop(first, members, step_body, 0)

    barrier = pltpu.get_barrier_semaphore()
    for distance in range(parts):

        def greet(step):
            row, col, _ = partner(distance, step)
            pl.semaphore_signal(barrier, inc=1, device_id=(row, col), device_id_type=MESH)

        each(1 if distance == 0 else 0, greet)

    def wait_bytes(ref, sem):
        pltpu.make_async_copy(ref, ref, sem).wait()

    def remote(source, target, send_sem, recv_sem, row, col):
        pltpu.make_async_remote_copy(
            src_ref=source,
            dst_ref=target,
            send_sem=send_sem,
            recv_sem=recv_sem,
            device_id=(row, col),
            device_id_type=MESH,
        ).start()

    row_at = pl.multiple_of(my_row * rows, rows)
    near_at = pl.multiple_of(lax.rem(my_row, row_part) * rows, rows)
    col_at = pl.multiple_of(my_col * cols, cols)

    def panels(chunk, place):
        return pl.ds(chunk * wide + place * piece, piece)

    def send_panels(section, chunk):
        spot = pl.ds(chunk * piece, piece)
        if section == 0:
            a_to = recv_a.at[spot, pl.ds(near_at, rows), pl.ds(col_at, cols)]
            b_to = recv_b.at[spot, pl.ds(row_at, rows), pl.ds(col_at, cols)]

            def far(distance, step):
                row, col, place = partner(distance, step)
                source = send_ab.at[0, 1, panels(chunk, place)]
                remote(
                    source, b_to, b_send_sem.at[distance], b_recv_sem.at[chunk], row, col
                )

            def near(step):
                row, col, place = partner(0, step)
                source = send_ab.at[0, 0, panels(chunk, place)]
                remote(source, a_to, a_send_sem, a_recv_sem.at[chunk], row, col)

            for distance in range(parts - 1, -1, -1):
                each(1 if distance == 0 else 0, functools.partial(far, distance))
            each(1, near)
            own = panels(chunk, my_place)
            pltpu.make_async_copy(send_ab.at[0, 0, own], a_to, a_recv_sem.at[chunk]).start()
            pltpu.make_async_copy(send_ab.at[0, 1, own], b_to, b_recv_sem.at[chunk]).start()
        else:
            to = recv_ab.at[:, spot, pl.ds(near_at, rows), pl.ds(col_at, cols)]

            def both(step):
                row, col, place = partner(0, step)
                source = send_ab.at[1, :, panels(chunk, place)]
                remote(source, to, ab_send_sem, ab_recv_sem.at[chunk], row, col)

            each(1, both)
            own = send_ab.at[1, :, panels(chunk, my_place)]
            pltpu.make_async_copy(own, to, ab_recv_sem.at[chunk]).start()

    def wait_panels(section, chunk):
        spot = pl.ds(chunk * piece, piece)
        if section == 0:
            wait_bytes(recv_a.at[spot], a_recv_sem.at[chunk])
            wait_bytes(recv_b.at[spot], b_recv_sem.at[chunk])
        else:
            wait_bytes(recv_ab.at[:, spot], ab_recv_sem.at[chunk])

    def send_products(section, chunk):
        spot = pl.ds(chunk * piece, piece)
        lands = panels(chunk, my_place)

        def refs_of(row, col):
            to_row = row if section == 1 else lax.rem(row, row_part)
            at = pl.ds(pl.multiple_of(to_row * rows, rows), rows)
            along = pl.ds(pl.multiple_of(col * cols, cols), cols)
            if section == 0:
                return send_x0.at[spot, at, along], recv_x0.at[lands]
            return send_x1.at[spot, at, along], recv_x1.at[my_group, lands]

        def other(distance, step):
            row, col, _ = partner(distance, step)
            source, target = refs_of(row, col)
            remote(
                source,
                target,
                x_send_sem.at[section, distance],
                x_recv_sem.at[section, chunk],
                row,
                col,
            )

        for distance in range(parts - 1 if section == 1 else 0, -1, -1):
            each(1 if distance == 0 else 0, functools.partial(other, distance))
        source, target = refs_of(my_row, my_col)
        pltpu.make_async_copy(source, target, x_recv_sem.at[section, chunk]).start()

    def prepare(section):
        for block in range(4):
            span = slice(block * hidden, (block + 1) * hidden)
            turned = held["panel_weight"][section, :, span].astype(jnp.float32).T
            turned = turned.astype(jnp.bfloat16)
            biases = held["panel_bias"][pl.ds(section, 1), span]
            biases = jnp.broadcast_to(biases, (cols, hidden)).T
            for chunk in range(chunks):
                to = pl.ds((chunk * 4 + block) * wide, wide)
                weight_t[section, to, :] = turned[chunk * wide : (chunk + 1) * wide]
                bias_t[section, to, :] = biases[chunk * wide : (chunk + 1) * wide]

    def prepare_affine(section):
        for at, name in enumerate(("hidden_gain", "hidden_shift")):
            line = held[name][pl.ds(section, 1), :]
            affine_t[section, at] = jnp.broadcast_to(line, (cols, hidden)).T

    def norm_row(section, values):
        return normalize(
            values,
            1,
            PAIR_EPSILON,
            held["pair_gain"][pl.ds(section, 1), :],
            held["pair_shift"][pl.ds(section, 1), :],
        )

    early = [NAMES.index(name) for name in ("pair", "pair_gain", "pair_shift")]
    for at in early:
        loads[at].wait()

    def first_norm(r, carry):
        normed_ref[r] = norm_row(0, held["pair"][r])
        return carry

    lax.fori_loop(0, rows, first_norm, 0, unroll=min(rows, 16))
    for at in range(count):
        if at not in early:
            loads[at].wait()
    prepare(0)
    col_mask = held["mask"][pl.ds(my_col, 1), :].astype(jnp.float32)

    for section in range(2):
        current = held["pair"] if section == 0 else out_ref
        def make(chunk):

            def project(r, carry):
                span = pl.ds(chunk * 4 * wide, 4 * wide)
                features = lax.dot_general(
                    weight_t[section, span, :],
                    normed_ref[r],
                    (((1,), (1,)), ((), ())),
                    preferred_element_type=jnp.float32,
                )
                features = features + bias_t[section, span, :]
                mask = col_mask * mask_smem[my_row * rows + r].astype(jnp.float32)
                for which in range(2):
                    at = 2 * which * wide
                    panel = mask * jax.nn.sigmoid(features[at : at + wide])
                    panel = panel * features[at + wide : at + 2 * wide]
                    stage[which, pl.ds(r, wide, stride=rows), :] = panel
                return carry

            lax.fori_loop(0, rows, project, 0, unroll=min(rows, 16))
            for which in range(2):
                send_ab[section, which, pl.ds(chunk * wide, wide)] = (
                    stage[which].astype(jnp.bfloat16).reshape(wide, rows, cols)
                )
            if section == 0 and chunk == 0:
                pl.semaphore_wait(barrier, devices - 1)
            send_panels(section, chunk)

        def gates(r, carry):
            gate[r] = jax.nn.sigmoid(
                jnp.dot(
                    normed_ref[r],
                    held["gate_weight"][section],
                    preferred_element_type=jnp.float32,
                )
                + held["gate_bias"][pl.ds(section, 1), :]
            )
            return carry

        def multiply(chunk):
            wait_panels(section, chunk)
            for h in range(chunk * piece, (chunk + 1) * piece):
                if section == 0:
                    left, right, along, to = recv_a[h], recv_b[h], 1, send_x0
                else:
                    left, right, along, to = recv_ab[0, h], recv_ab[1, h], 0, send_x1
                to[h] = lax.dot_general(
                    left,
                    right,
                    (((along,), (along,)), ((), ())),
                    preferred_element_type=jnp.float32,
                ).astype(jnp.bfloat16)
            send_products(section, chunk)

        lead = chunks if section == 0 else min(LEAD, chunks)
        for chunk in range(lead):
            make(chunk)
        if section == 0:
            lax.fori_loop(0, rows, gates, 0, unroll=min(rows, 16))
            prepare(1)
            prepare_affine(0)
            prepare_affine(1)
        for chunk in range(chunks):
            multiply(chunk)
            if chunk + lead < chunks:
                make(chunk + lead)
        if section == 1:
            lax.fori_loop(0, rows, gates, 0, unroll=min(rows, 16))
        for chunk in range(chunks):
            spot = pl.ds(chunk * wide, wide)
            if section == 0:
                wait_bytes(recv_x0.at[spot], x_recv_sem.at[0, chunk])
                got = recv_x0[spot].astype(jnp.float32)
            else:
                wait_bytes(recv_x1.at[:, spot], x_recv_sem.at[1, chunk])
                got = recv_x1[0, spot].astype(jnp.float32)
                for other in range(1, parts):
                    got = got + recv_x1[other, spot].astype(jnp.float32)
            stage_x[pl.ds(chunk * wide * rows, wide * rows), :] = got.reshape(wide * rows, cols)

        def finish(r, carry):
            normed = normalize(
                stage_x[pl.ds(r, hidden, stride=rows), :],
                0,
                HIDDEN_EPSILON,
                affine_t[section, 0],
                affine_t[section, 1],
            )
            projected = lax.dot_general(
                normed,
                held["output_weight"][section],
                (((0,), (0,)), ((), ())),
                preferred_element_type=jnp.float32,
            )
            projected = projected + held["output_bias"][pl.ds(section, 1), :]
            updated = current[r] + gate[r] * projected
            out_ref[r] = updated
            if section == 0:
                normed_ref[r] = norm_row(1, updated)
            return carry

        lax.fori_loop(0, rows, finish, 0, unroll=min(rows, 16))

    one = hidden - per_slot
    wait_bytes(send_ab.at[0, 0, pl.ds(0, one)], a_send_sem)
    wait_bytes(send_ab.at[1, :, pl.ds(0, one)], ab_send_sem)
    for distance in range(parts):
        amount = one if distance == 0 else hidden
        wait_bytes(send_ab.at[0, 1, pl.ds(0, amount)], b_send_sem.at[distance])
        wait_bytes(send_ab.at[0, 1, pl.ds(0, amount)], x_send_sem.at[1, distance])
    wait_bytes(recv_x0.at[pl.ds(0, one)], x_send_sem.at[0, 0])


def local(row_total, col_total, pair_rep, residue_mask, *parameters):
    rows, cols, channels = pair_rep.shape
    hidden = parameters[2].shape[2] // 4
    parts = max(2, row_total * col_total // hidden)
    members = row_total * col_total // parts
    per_slot = hidden // members
    chunks = min(CHUNKS, per_slot)
    wide = hidden // chunks
    total = row_total * rows
    part = total // parts
    sizes = (rows, cols, hidden, row_total, col_total, parts, chunks)
    bf16, f32 = jnp.bfloat16, jnp.float32
    dma = pltpu.SemaphoreType.DMA
    arrays = (pair_rep, residue_mask.reshape(col_total, cols), *parameters)
    return pl.pallas_call(
        functools.partial(kernel, sizes),
        out_shape=jax.ShapeDtypeStruct((rows, cols, channels), f32),
        in_specs=[pl.BlockSpec(memory_space=pltpu.SMEM)]
        + [pl.BlockSpec(memory_space=pltpu.HBM)] * len(arrays),
        out_specs=pl.BlockSpec(memory_space=pltpu.VMEM),
        scratch_shapes=[pltpu.VMEM(array.shape, array.dtype) for array in arrays]
        + [
            pltpu.VMEM((2, 4 * hidden, channels), bf16),
            pltpu.VMEM((2, 4 * hidden, cols), f32),
            pltpu.VMEM((2, 2, hidden, cols), f32),
            pltpu.VMEM((rows, cols, channels), bf16),
            pltpu.VMEM((2, wide * rows, cols), f32),
            pltpu.VMEM((hidden * rows, cols), f32),
            pltpu.VMEM((rows, cols, channels), f32),
            pltpu.VMEM((2, 2, hidden, rows, cols), bf16),
            pltpu.VMEM((per_slot, part, total), bf16),
            pltpu.VMEM((per_slot, total, total), bf16),
            pltpu.VMEM((2, per_slot, part, total), bf16),
            pltpu.VMEM((per_slot, part, total), bf16),
            pltpu.VMEM((per_slot, total, total), bf16),
            pltpu.VMEM((hidden, rows, cols), bf16),
            pltpu.VMEM((parts, hidden, rows, cols), bf16),
            dma((len(arrays),)),
            dma(()),
            dma((chunks,)),
            dma((parts,)),
            dma((chunks,)),
            dma(()),
            dma((chunks,)),
            dma((2, parts)),
            dma((2, chunks)),
        ],
        compiler_params=pltpu.CompilerParams(collective_id=0, has_side_effects=True),
    )(residue_mask, *arrays)


def solution(mesh):
    return jax.shard_map(
        functools.partial(local, mesh.shape["row"], mesh.shape["ch"]),
        mesh=mesh,
        in_specs=(P("row", "ch", None), P(), P(), P(), P(), P(), P(), P(), P(), P(), P(), P()),
        out_specs=P("row", "ch", None),
        check_vma=False,
    )
```

```python
import functools

import jax
import jax.numpy as jnp
from jax import lax
from jax.experimental import pallas as pl
from jax.experimental.pallas import tpu as pltpu
from jax.sharding import PartitionSpec as P

PAIR_EPSILON = 1e-05
HIDDEN_EPSILON = 1.0
MESH = pl.DeviceIdType.MESH
CHUNKS = 4
LEAD = 3
NAMES = (
    "pair",
    "mask",
    "pair_gain",
    "pair_shift",
    "panel_weight",
    "panel_bias",
    "gate_weight",
    "gate_bias",
    "hidden_gain",
    "hidden_shift",
    "output_weight",
    "output_bias",
)


def normalize(values, axis, epsilon, gain, shift):
    offset = values - jnp.mean(values, axis=axis, keepdims=True)
    spread = jnp.mean(offset * offset, axis=axis, keepdims=True)
    return (offset * lax.rsqrt(spread + epsilon) * gain + shift).astype(jnp.bfloat16)


def kernel(sizes, mask_smem, *refs):
    rows, cols, hidden, row_total, col_total, parts, chunks = sizes
    count = len(NAMES)
    sources = dict(zip(NAMES, refs[:count]))
    out_ref = refs[count]
    held = dict(zip(NAMES, refs[count + 1 : 2 * count + 1]))
    (
        weight_t,
        bias_t,
        affine_t,
        normed_ref,
        stage,
        stage_x,
        gate,
        send_ab,
        recv_a,
        recv_b,
        recv_ab,
        send_x0,
        send_x1,
        recv_x0,
        recv_x1,
        load_sem,
        a_send_sem,
        a_recv_sem,
        b_send_sem,
        b_recv_sem,
        ab_send_sem,
        ab_recv_sem,
        x_send_sem,
        x_recv_sem,
    ) = refs[2 * count + 1 :]
    devices = row_total * col_total
    row_part = row_total // parts
    members = row_part * col_total
    per_slot = hidden // members
    piece = per_slot // chunks
    wide = hidden // chunks
    total = row_total * rows
    part = total // parts
    my_row = lax.axis_index("row")
    my_col = lax.axis_index("ch")
    my_group = my_row // row_part
    my_place = lax.rem(my_row, row_part) * col_total + my_col

    loads = [
        pltpu.make_async_copy(sources[name], held[name], load_sem.at[at])
        for at, name in enumerate(NAMES)
    ]
    for load in loads:
        load.start()

    def partner(distance, step):
        group = lax.rem(my_group + distance, parts)
        place = lax.rem(my_place + step, members)
        return group * row_part + place // col_total, lax.rem(place, col_total), place

    def each(first, body):
        def step_body(step, carry):
            body(step)
            return carry

        steps = members - first
        unroll = max(d for d in (1, 4, 5) if steps % d == 0)
        lax.fori_loop(first, members, step_body, 0, unroll=unroll)

    barrier = pltpu.get_barrier_semaphore()
    for distance in range(parts):

        def greet(step):
            row, col, _ = partner(distance, step)
            pl.semaphore_signal(barrier, inc=1, device_id=(row, col), device_id_type=MESH)

        each(1 if distance == 0 else 0, greet)

    def wait_bytes(ref, sem):
        pltpu.make_async_copy(ref, ref, sem).wait()

    def remote(source, target, send_sem, recv_sem, row, col):
        pltpu.make_async_remote_copy(
            src_ref=source,
            dst_ref=target,
            send_sem=send_sem,
            recv_sem=recv_sem,
            device_id=(row, col),
            device_id_type=MESH,
        ).start()

    row_at = pl.multiple_of(my_row * rows, rows)
    near_at = pl.multiple_of(lax.rem(my_row, row_part) * rows, rows)
    col_at = pl.multiple_of(my_col * cols, cols)

    def panels(chunk, place):
        return pl.ds(chunk * wide + place * piece, piece)

    def send_panels(section, chunk):
        spot = pl.ds(chunk * piece, piece)
        if section == 0:
            a_to = recv_a.at[spot, pl.ds(near_at, rows), pl.ds(col_at, cols)]
            b_to = recv_b.at[spot, pl.ds(row_at, rows), pl.ds(col_at, cols)]

            def far(distance, step):
                row, col, place = partner(distance, step)
                source = send_ab.at[0, 1, panels(chunk, place)]
                remote(
                    source, b_to, b_send_sem.at[distance], b_recv_sem.at[chunk], row, col
                )

            def near(step):
                row, col, place = partner(0, step)
                source = send_ab.at[0, 0, panels(chunk, place)]
                remote(source, a_to, a_send_sem, a_recv_sem.at[chunk], row, col)

            for distance in range(parts - 1, -1, -1):
                each(1 if distance == 0 else 0, functools.partial(far, distance))
            each(1, near)
            own = panels(chunk, my_place)
            pltpu.make_async_copy(send_ab.at[0, 0, own], a_to, a_recv_sem.at[chunk]).start()
            pltpu.make_async_copy(send_ab.at[0, 1, own], b_to, b_recv_sem.at[chunk]).start()
        else:
            to = recv_ab.at[:, spot, pl.ds(near_at, rows), pl.ds(col_at, cols)]

            def both(step):
                row, col, place = partner(0, step)
                source = send_ab.at[1, :, panels(chunk, place)]
                remote(source, to, ab_send_sem, ab_recv_sem.at[chunk], row, col)

            each(1, both)
            own = send_ab.at[1, :, panels(chunk, my_place)]
            pltpu.make_async_copy(own, to, ab_recv_sem.at[chunk]).start()

    def wait_panels(section, chunk):
        spot = pl.ds(chunk * piece, piece)
        if section == 0:
            wait_bytes(recv_a.at[spot], a_recv_sem.at[chunk])
            wait_bytes(recv_b.at[spot], b_recv_sem.at[chunk])
        else:
            wait_bytes(recv_ab.at[:, spot], ab_recv_sem.at[chunk])

    def send_products(section, chunk):
        spot = pl.ds(chunk * piece, piece)
        lands = panels(chunk, my_place)

        def refs_of(row, col):
            to_row = row if section == 1 else lax.rem(row, row_part)
            at = pl.ds(pl.multiple_of(to_row * rows, rows), rows)
            along = pl.ds(pl.multiple_of(col * cols, cols), cols)
            if section == 0:
                return send_x0.at[spot, at, along], recv_x0.at[lands]
            return send_x1.at[spot, at, along], recv_x1.at[my_group, lands]

        def other(distance, step):
            row, col, _ = partner(distance, step)
            source, target = refs_of(row, col)
            remote(
                source,
                target,
                x_send_sem.at[section, distance],
                x_recv_sem.at[section, chunk],
                row,
                col,
            )

        for distance in range(parts - 1 if section == 1 else 0, -1, -1):
            each(1 if distance == 0 else 0, functools.partial(other, distance))
        source, target = refs_of(my_row, my_col)
        pltpu.make_async_copy(source, target, x_recv_sem.at[section, chunk]).start()

    def prepare(section):
        for block in range(4):
            span = slice(block * hidden, (block + 1) * hidden)
            turned = held["panel_weight"][section, :, span].astype(jnp.float32).T
            turned = turned.astype(jnp.bfloat16)
            biases = held["panel_bias"][pl.ds(section, 1), span]
            biases = jnp.broadcast_to(biases, (cols, hidden)).T
            for chunk in range(chunks):
                to = pl.ds((chunk * 4 + block) * wide, wide)
                weight_t[section, to, :] = turned[chunk * wide : (chunk + 1) * wide]
                bias_t[section, to, :] = biases[chunk * wide : (chunk + 1) * wide]

    def prepare_affine(section):
        for at, name in enumerate(("hidden_gain", "hidden_shift")):
            line = held[name][pl.ds(section, 1), :]
            affine_t[section, at] = jnp.broadcast_to(line, (cols, hidden)).T

    def norm_row(section, values):
        return normalize(
            values,
            1,
            PAIR_EPSILON,
            held["pair_gain"][pl.ds(section, 1), :],
            held["pair_shift"][pl.ds(section, 1), :],
        )

    early = [NAMES.index(name) for name in ("pair", "pair_gain", "pair_shift")]
    for at in early:
        loads[at].wait()

    def first_norm(r, carry):
        normed_ref[r] = norm_row(0, held["pair"][r])
        return carry

    lax.fori_loop(0, rows, first_norm, 0, unroll=min(rows, 16))
    for at in range(count):
        if at not in early:
            loads[at].wait()
    prepare(0)
    col_mask = held["mask"][pl.ds(my_col, 1), :].astype(jnp.float32)

    for section in range(2):
        current = held["pair"] if section == 0 else out_ref
        def make(chunk):

            def project(r, carry):
                span = pl.ds(chunk * 4 * wide, 4 * wide)
                features = lax.dot_general(
                    weight_t[section, span, :],
                    normed_ref[r],
                    (((1,), (1,)), ((), ())),
                    preferred_element_type=jnp.float32,
                )
                features = features + bias_t[section, span, :]
                mask = col_mask * mask_smem[my_row * rows + r].astype(jnp.float32)
                for which in range(2):
                    at = 2 * which * wide
                    panel = mask * jax.nn.sigmoid(features[at : at + wide])
                    panel = panel * features[at + wide : at + 2 * wide]
                    stage[which, pl.ds(r, wide, stride=rows), :] = panel
                return carry

            lax.fori_loop(0, rows, project, 0, unroll=min(rows, 16))
            for which in range(2):
                send_ab[section, which, pl.ds(chunk * wide, wide)] = (
                    stage[which].astype(jnp.bfloat16).reshape(wide, rows, cols)
                )
            if section == 0 and chunk == 0:
                pl.semaphore_wait(barrier, devices - 1)
            send_panels(section, chunk)

        def gates(r, carry):
            gate[r] = jax.nn.sigmoid(
                jnp.dot(
                    normed_ref[r],
                    held["gate_weight"][section],
                    preferred_element_type=jnp.float32,
                )
                + held["gate_bias"][pl.ds(section, 1), :]
            )
            return carry

        def multiply(chunk):
            wait_panels(section, chunk)
            for h in range(chunk * piece, (chunk + 1) * piece):
                if section == 0:
                    left, right, along, to = recv_a[h], recv_b[h], 1, send_x0
                else:
                    left, right, along, to = recv_ab[0, h], recv_ab[1, h], 0, send_x1
                to[h] = lax.dot_general(
                    left,
                    right,
                    (((along,), (along,)), ((), ())),
                    preferred_element_type=jnp.float32,
                ).astype(jnp.bfloat16)
            send_products(section, chunk)

        lead = chunks if section == 0 else min(LEAD, chunks)
        for chunk in range(lead):
            make(chunk)
        if section == 0:
            lax.fori_loop(0, rows, gates, 0, unroll=min(rows, 16))
            prepare(1)
            prepare_affine(0)
            prepare_affine(1)
        for chunk in range(chunks):
            multiply(chunk)
            if chunk + lead < chunks:
                make(chunk + lead)
        if section == 1:
            lax.fori_loop(0, rows, gates, 0, unroll=min(rows, 16))
        for chunk in range(chunks):
            spot = pl.ds(chunk * wide, wide)
            if section == 0:
                wait_bytes(recv_x0.at[spot], x_recv_sem.at[0, chunk])
                got = recv_x0[spot].astype(jnp.float32)
            else:
                wait_bytes(recv_x1.at[:, spot], x_recv_sem.at[1, chunk])
                got = recv_x1[0, spot].astype(jnp.float32)
                for other in range(1, parts):
                    got = got + recv_x1[other, spot].astype(jnp.float32)
            stage_x[pl.ds(chunk * wide * rows, wide * rows), :] = got.reshape(wide * rows, cols)

        def finish(r, carry):
            normed = normalize(
                stage_x[pl.ds(r, hidden, stride=rows), :],
                0,
                HIDDEN_EPSILON,
                affine_t[section, 0],
                affine_t[section, 1],
            )
            projected = lax.dot_general(
                normed,
                held["output_weight"][section],
                (((0,), (0,)), ((), ())),
                preferred_element_type=jnp.float32,
            )
            projected = projected + held["output_bias"][pl.ds(section, 1), :]
            updated = current[r] + gate[r] * projected
            out_ref[r] = updated
            if section == 0:
                normed_ref[r] = norm_row(1, updated)
            return carry

        lax.fori_loop(0, rows, finish, 0, unroll=min(rows, 16))

    one = hidden - per_slot
    wait_bytes(send_ab.at[0, 0, pl.ds(0, one)], a_send_sem)
    wait_bytes(send_ab.at[1, :, pl.ds(0, one)], ab_send_sem)
    for distance in range(parts):
        amount = one if distance == 0 else hidden
        wait_bytes(send_ab.at[0, 1, pl.ds(0, amount)], b_send_sem.at[distance])
        wait_bytes(send_ab.at[0, 1, pl.ds(0, amount)], x_send_sem.at[1, distance])
    wait_bytes(recv_x0.at[pl.ds(0, one)], x_send_sem.at[0, 0])


def local(row_total, col_total, pair_rep, residue_mask, *parameters):
    rows, cols, channels = pair_rep.shape
    hidden = parameters[2].shape[2] // 4
    parts = max(2, row_total * col_total // hidden)
    members = row_total * col_total // parts
    per_slot = hidden // members
    chunks = min(CHUNKS, per_slot)
    wide = hidden // chunks
    total = row_total * rows
    part = total // parts
    sizes = (rows, cols, hidden, row_total, col_total, parts, chunks)
    bf16, f32 = jnp.bfloat16, jnp.float32
    dma = pltpu.SemaphoreType.DMA
    arrays = (pair_rep, residue_mask.reshape(col_total, cols), *parameters)
    return pl.pallas_call(
        functools.partial(kernel, sizes),
        out_shape=jax.ShapeDtypeStruct((rows, cols, channels), f32),
        in_specs=[pl.BlockSpec(memory_space=pltpu.SMEM)]
        + [pl.BlockSpec(memory_space=pltpu.HBM)] * len(arrays),
        out_specs=pl.BlockSpec(memory_space=pltpu.VMEM),
        scratch_shapes=[pltpu.VMEM(array.shape, array.dtype) for array in arrays]
        + [
            pltpu.VMEM((2, 4 * hidden, channels), bf16),
            pltpu.VMEM((2, 4 * hidden, cols), f32),
            pltpu.VMEM((2, 2, hidden, cols), f32),
            pltpu.VMEM((rows, cols, channels), bf16),
            pltpu.VMEM((2, wide * rows, cols), f32),
            pltpu.VMEM((hidden * rows, cols), f32),
            pltpu.VMEM((rows, cols, channels), f32),
            pltpu.VMEM((2, 2, hidden, rows, cols), bf16),
            pltpu.VMEM((per_slot, part, total), bf16),
            pltpu.VMEM((per_slot, total, total), bf16),
            pltpu.VMEM((2, per_slot, part, total), bf16),
            pltpu.VMEM((per_slot, part, total), bf16),
            pltpu.VMEM((per_slot, total, total), bf16),
            pltpu.VMEM((hidden, rows, cols), bf16),
            pltpu.VMEM((parts, hidden, rows, cols), bf16),
            dma((len(arrays),)),
            dma(()),
            dma((chunks,)),
            dma((parts,)),
            dma((chunks,)),
            dma(()),
            dma((chunks,)),
            dma((2, parts)),
            dma((2, chunks)),
        ],
        compiler_params=pltpu.CompilerParams(collective_id=0, has_side_effects=True),
    )(residue_mask, *arrays)


def solution(mesh):
    return jax.shard_map(
        functools.partial(local, mesh.shape["row"], mesh.shape["ch"]),
        mesh=mesh,
        in_specs=(P("row", "ch", None), P(), P(), P(), P(), P(), P(), P(), P(), P(), P(), P()),
        out_specs=P("row", "ch", None),
        check_vma=False,
    )
```
